16 devices in a mesh: vp: 16 (over z, y, x, core).
Axes of the slice: x: 2, y: 2, z: 2, core: 2. Of those that a mesh axis runs over, the one named last changes fastest.
Arguments:
- hidden: bfloat16 [256, 1024], replicated
- ln_weight: bfloat16 [1024], replicated
- ln_bias: bfloat16 [1024], replicated
- embedding: bfloat16 [250880, 1024], P('vp')
- temperature: float32 [], replicated
- cand_ids: int32 [256, 128], replicated
Outputs:
- output 1: float32 [256, 250880], P(None, 'vp')
- output 2: float32 [256, 128], replicated
All inputs are finite; a program needn't handle non-finite values.
Results may differ from the reference program's by a relative error of at most 0.001.
Values sent between devices are 32-bit elements.
A program may use at most 1 GiB of HBM per device.

```python
import jax
import jax.numpy as jnp
from jax import lax

BATCH = 256
HIDDEN = 1024
VOCAB = 250880
CANDS = 128
CLUSTER_IDS = VOCAB // 64


def hot_scales(key_rows):
    hot_draw = jax.random.randint(key_rows, (VOCAB,), 0, 64)
    return jnp.where(hot_draw == 0, 3.0, 1.0).astype(jnp.float32)


def draw_candidates(key_cand):
    k_center, k_pick, k_offset, k_spread = jax.random.split(key_cand, 4)
    centers = jax.random.randint(k_center, (3,), 0, VOCAB - CLUSTER_IDS)
    pick_idx = jax.random.randint(k_pick, (BATCH, CANDS), 0, 3)
    offsets = jax.random.randint(k_offset, (BATCH, CANDS), 0, CLUSTER_IDS)
    spread = jax.random.randint(k_spread, (BATCH, CANDS), 0, VOCAB)
    clustered = jnp.take(centers, pick_idx) + offsets
    column = jnp.arange(CANDS)[None, :]
    cand_ids = jnp.where(column % 4 == 3, spread, clustered)
    cand_ids = cand_ids.at[0, 0].set(0).at[BATCH - 1, CANDS - 1].set(VOCAB - 1)
    return cand_ids.astype(jnp.int32)


def setup_inputs(seed: int = 0) -> dict:
    root_key = jax.random.key(seed)
    k_hidden, k_weight, k_bias, k_embed, k_hot, k_temp, k_cand = jax.random.split(root_key, 7)
    hidden = jax.random.normal(k_hidden, (BATCH, HIDDEN), jnp.float32)
    ln_weight = 1.0 + 0.5 * jax.random.normal(k_weight, (HIDDEN,), jnp.float32)
    ln_bias = 0.5 * jax.random.normal(k_bias, (HIDDEN,), jnp.float32)
    row_gain = hot_scales(k_hot) * (HIDDEN ** -0.5)
    embedding = jax.random.normal(k_embed, (VOCAB, HIDDEN), jnp.float32) * row_gain[:, None]
    temperature = jax.random.uniform(k_temp, (), jnp.float32, minval=0.8, maxval=1.25)
    return {
        "hidden": hidden.astype(jnp.bfloat16),
        "ln_weight": ln_weight.astype(jnp.bfloat16),
        "ln_bias": ln_bias.astype(jnp.bfloat16),
        "embedding": embedding.astype(jnp.bfloat16),
        "temperature": temperature,
        "cand_ids": draw_candidates(k_cand),
    }


def reference(hidden, ln_weight, ln_bias, embedding, temperature, cand_ids):
    hidden_f32 = hidden.astype(jnp.float32)
    row_mean = jnp.mean(hidden_f32, axis=-1, keepdims=True)
    centered = hidden_f32 - row_mean
    row_var = jnp.mean(centered * centered, axis=-1, keepdims=True)
    scaled = centered * lax.rsqrt(row_var + 1e-5)
    normed = (scaled * ln_weight.astype(jnp.float32) + ln_bias.astype(jnp.float32)).astype(jnp.bfloat16)
    logits = lax.dot_general(normed, embedding, (((1,), (1,)), ((), ())), preferred_element_type=jnp.float32) / temperature
    row_max = jnp.max(logits, axis=1, keepdims=True)
    exp_sum = jnp.sum(jnp.exp(logits - row_max), axis=1, keepdims=True)
    logprobs = logits - (row_max + jnp.log(exp_sum))
    cand_lp = jnp.take_along_axis(logprobs, cand_ids, axis=1)
    return logprobs, cand_lp
```

```python
import functools

import jax
import jax.numpy as jnp
from jax import lax
from jax.sharding import PartitionSpec as P
from jax.experimental import pallas as pl
from jax.experimental.pallas import tpu as pltpu

N = 16
NV = 15680
D = 1024
B = 256
J = 128
RB = B // N
R = 768
NMAIN = 20
TAIL = NV - NMAIN * R
GX = 2
LOG2E = 1.4426950408889634
MESH = pl.DeviceIdType.MESH


def chunk_list():
    out = [(c * R, R) for c in range(NMAIN)]
    out.append((NMAIN * R, TAIL))
    return out


def lane_gather(x, idx):
    dn = lax.GatherDimensionNumbers(
        offset_dims=(), collapsed_slice_dims=(1,), start_index_map=(1,),
        operand_batching_dims=(0,), start_indices_batching_dims=(0,))
    return lax.gather(x, idx[:, :, None], dn, slice_sizes=(1, 1),
                      mode=lax.GatherScatterMode.PROMISE_IN_BOUNDS)


def local_chunk_stats(z_ref, o, r, k2, m, s):
    u = z_ref[pl.ds(o, r), :].reshape(r // 8, 8, B)
    mn = jnp.maximum(m, jnp.max(u, axis=0))
    p = jnp.exp2((u - mn[None]) * k2[None])
    return mn, s * jnp.exp2((m - mn) * k2) + jnp.sum(p, axis=0)


def local_chunk_gather(z_ref, o, r, loc, acc_ref, scr):
    tiles = [(o + k * 128, o // 128 + k, 0) for k in range(r // 128)]
    if r % 128:
        tiles.append((NV - 128, NV // 128, 128 - NV % 128))
    for ih in range(2):
        for k, (ro, _, _) in enumerate(tiles):
            scr[ih, :, k * 128:(k + 1) * 128] = z_ref[pl.ds(ro, 128), ih * 128:(ih + 1) * 128].T
        for g in range(16):
            r0 = ih * 128 + g * 8
            cv = loc[r0:r0 + 8, :]
            ti = cv >> 7
            li = cv & 127
            acc = acc_ref[r0:r0 + 8, :]
            for k, (_, tid, sh) in enumerate(tiles):
                idx = li if sh == 0 else (li + sh) & 127
                got = lane_gather(scr[ih, g * 8:g * 8 + 8, k * 128:(k + 1) * 128], idx)
                hit = ti == tid
                if sh:
                    hit = hit & (cv < NV)
                acc = jnp.where(hit, got, acc)
            acc_ref[r0:r0 + 8, :] = acc


def stream_kernel(*refs):
    pl.run_scoped(
        functools.partial(stream_body, *refs),
        *[pltpu.ACC(mxu_id=mx)((h, B), jnp.float32) for mx in (0, 1) for h in (R // 2, R // 2, TAIL // 2)])


def stream_body(t_ref, x_hbm, w_ref, b_ref, e_hbm, c_hbm, z_ref, ms_ref, cacc, cbuf,
                ebuf, xbuf, abuf, scr, esem, xsem, csem,
                a00, a01, a0t, a10, a11, a1t):
    me = lax.axis_index("vp")
    chunks = chunk_list()
    accs = [[a00, a01, a0t], [a10, a11, a1t]]

    xcp = pltpu.make_async_copy(x_hbm, xbuf, xsem)
    xcp.start()
    ccp = pltpu.make_async_copy(c_hbm, cbuf, csem)
    ecps = []
    for c, (o, r) in enumerate(chunks):
        cp = pltpu.make_async_copy(e_hbm.at[pl.ds(o, r)], ebuf.at[pl.ds(o, r)], esem.at[c])
        cp.start()
        ecps.append(cp)
        if c == 0:
            ccp.start()

    xcp.wait()
    wv = w_ref[...].astype(jnp.float32)
    bv = b_ref[...].astype(jnp.float32)
    for g in range(0, B, 64):
        x = xbuf[g:g + 64, :].astype(jnp.float32)
        mu = jnp.sum(x, axis=1, keepdims=True) * (1.0 / D)
        xc = x - mu
        var = jnp.sum(xc * xc, axis=1, keepdims=True) * (1.0 / D)
        abuf[g:g + 64, :] = (xc * lax.rsqrt(var + 1e-5) * wv + bv).astype(jnp.bfloat16)

    k2 = (1.0 / t_ref[...]) * LOG2E
    ccp.wait()
    cbuf[...] = cbuf[...] - me * NV
    cacc[...] = jnp.zeros_like(cacc)
    m = jnp.full((8, B), -jnp.inf, jnp.float32)
    s = jnp.zeros((8, B), jnp.float32)

    def issue(c):
        o, r = chunks[c]
        slot = 2 if r == TAIL else c % 2
        h = r // 2
        for kt in range(4):
            for mx in range(2):
                pltpu.matmul_push_rhs(abuf[:, kt * 256:(kt + 1) * 256], staging_register=kt % 2, mxu_index=mx, transpose=True)
            for mx in range(2):
                pltpu.matmul_acc_lhs(accs[mx][slot], ebuf[pl.ds(o + mx * h, h), kt * 256:(kt + 1) * 256], load_staged_rhs=kt % 2)

    def pop(c):
        o, r = chunks[c]
        slot = 2 if r == TAIL else c % 2
        h = r // 2
        for mx in range(2):
            z_ref[pl.ds(o + mx * h, h), :] = pltpu.matmul_pop(accs[mx][slot])

    ns = len(chunks) - GX
    for c in range(len(chunks) + 1):
        if c < len(chunks):
            ecps[c].wait()
            issue(c)
        if c >= 1:
            pop(c - 1)
        if 2 <= c < ns + 2:
            o, r = chunks[c - 2]
            m, s = local_chunk_stats(z_ref, o, r, k2, m, s)
            local_chunk_gather(z_ref, o, r, cbuf, cacc, scr)
    ms_ref[0] = m
    ms_ref[1] = s


def exchange_kernel(t_ref, z_ref, ms_ref, cacc_in, loc, lz_ref, q_ref,
                    scr, cacc, st_send, st_recv, rs_recv, ag_send, ag_recv,
                    st_ss, st_rs, rs_ss, rs_rs, ag_ss, ag_rs):
    me = lax.axis_index("vp")
    peers = [lax.rem(me + k, N) for k in range(1, N)]
    bar = pltpu.get_barrier_semaphore()
    for p in peers:
        pl.semaphore_signal(bar, inc=1, device_id=(p,), device_id_type=MESH)

    inv_t = 1.0 / t_ref[...]
    k2 = inv_t * LOG2E
    chunks = chunk_list()
    ns = len(chunks) - GX
    m, s = ms_ref[0], ms_ref[1]
    for o, r in chunks[ns:]:
        m, s = local_chunk_stats(z_ref, o, r, k2, m, s)
    mloc = jnp.max(m, axis=0, keepdims=True)
    sloc = jnp.sum(s * jnp.exp2((m - mloc) * k2), axis=0, keepdims=True)
    st_send[0:1, :] = mloc
    st_send[1:2, :] = sloc
    cacc[...] = cacc_in[...]
    for o, r in chunks[ns:]:
        local_chunk_gather(z_ref, o, r, loc, cacc, scr)
    pl.semaphore_wait(bar, N - 1)

    st = []
    for k in range(1, N):
        cp = pltpu.make_async_remote_copy(st_send, st_recv.at[k], st_ss.at[k], st_rs.at[k], device_id=(peers[k - 1],), device_id_type=MESH)
        cp.start()
        st.append(cp)
    rs = []
    for k in range(1, N):
        cp = pltpu.make_async_remote_copy(cacc.at[pl.ds(pl.multiple_of(peers[k - 1] * RB, RB), RB)], rs_recv.at[k], rs_ss.at[k], rs_rs.at[k],
                                          device_id=(peers[k - 1],), device_id_type=MESH)
        cp.start()
        rs.append(cp)
    for cp in st:
        cp.wait()
    mp = [mloc] + [st_recv[k, 0:1, :] for k in range(1, N)]
    sp = [sloc] + [st_recv[k, 1:2, :] for k in range(1, N)]
    mg = functools.reduce(jnp.maximum, mp)
    sg = functools.reduce(jnp.add, [b * jnp.exp2((a - mg) * k2) for a, b in zip(mp, sp)])
    lz = mg * inv_t + jnp.log(sg)
    lz_ref[...] = lz
    for cp in rs:
        cp.wait()
    tot = cacc[pl.ds(pl.multiple_of(me * RB, RB), RB), :]
    for k in range(1, N):
        tot = tot + rs_recv[k]
    ag_send[...] = tot
    ag = []
    for k in range(1, N):
        cp = pltpu.make_async_remote_copy(ag_send, ag_recv.at[pl.ds(pl.multiple_of(me * RB, RB), RB)], ag_ss.at[k], ag_rs.at[k],
                                          device_id=(peers[k - 1],), device_id_type=MESH)
        cp.start()
        ag.append(cp)
    cols = [jnp.broadcast_to(lz[:, ih * 128:(ih + 1) * 128], (128, 128)).T for ih in range(2)]
    for cp in ag:
        cp.wait()
    ag_recv[pl.ds(pl.multiple_of(me * RB, RB), RB), :] = tot
    for ih in range(2):
        q_ref[ih * 128:(ih + 1) * 128, :] = ag_recv[ih * 128:(ih + 1) * 128, :] * inv_t - cols[ih]


def solution(mesh):
    axis_name = mesh.axis_names[0]
    vm = pl.BlockSpec(memory_space=pltpu.VMEM)
    anyspec = pl.BlockSpec(memory_space=pl.ANY)
    nch = NMAIN + 1

    def per_device(hidden, ln_weight, ln_bias, emb_shard, temperature, cand_ids):
        t11 = temperature.reshape(1, 1)
        z, ms, cacc, loc = pl.pallas_call(
            stream_kernel,
            out_shape=[pltpu.VMEM((NV, B), jnp.float32), pltpu.VMEM((2, 8, B), jnp.float32),
                       pltpu.VMEM((B, J), jnp.float32), pltpu.VMEM((B, J), jnp.int32)],
            in_specs=[vm, anyspec, vm, vm, anyspec, anyspec],
            out_specs=[vm] * 4,
            scratch_shapes=[
                pltpu.VMEM((NV, D), jnp.bfloat16),
                pltpu.VMEM((B, D), jnp.bfloat16),
                pltpu.VMEM((B, D), jnp.bfloat16),
                pltpu.VMEM((2, 128, R), jnp.float32),
                pltpu.SemaphoreType.DMA((nch,)),
                pltpu.SemaphoreType.DMA,
                pltpu.SemaphoreType.DMA,
            ],
            compiler_params=pltpu.CompilerParams(vmem_limit_bytes=44 * 1024 * 1024),
        )(t11, hidden, ln_weight.reshape(1, D), ln_bias.reshape(1, D), emb_shard, cand_ids)
        pin = lambda a: pltpu.with_memory_space_constraint(a, pltpu.VMEM)
        lz, q = pl.pallas_call(
            exchange_kernel,
            out_shape=[pltpu.VMEM((1, B), jnp.float32), pltpu.VMEM((B, J), jnp.float32)],
            in_specs=[vm] * 5,
            out_specs=[vm] * 2,
            scratch_shapes=[
                pltpu.VMEM((2, 128, R), jnp.float32),
                pltpu.VMEM((B, J), jnp.float32),
                pltpu.VMEM((2, B), jnp.float32),
                pltpu.VMEM((N, 2, B), jnp.float32),
                pltpu.VMEM((N, RB, J), jnp.float32),
                pltpu.VMEM((RB, J), jnp.float32),
                pltpu.VMEM((B, J), jnp.float32),
                pltpu.SemaphoreType.DMA((N,)),
                pltpu.SemaphoreType.DMA((N,)),
                pltpu.SemaphoreType.DMA((N,)),
                pltpu.SemaphoreType.DMA((N,)),
                pltpu.SemaphoreType.DMA((N,)),
                pltpu.SemaphoreType.DMA((N,)),
            ],
            compiler_params=pltpu.CompilerParams(collective_id=0, has_side_effects=True, vmem_limit_bytes=24 * 1024 * 1024),
        )(t11, pin(z), pin(ms), pin(cacc), pin(loc))
        lp = z * (1.0 / temperature) - lz
        return lp.T, q

    return jax.shard_map(
        per_device,
        mesh=mesh,
        in_specs=(P(), P(), P(), P(axis_name, None), P(), P()),
        out_specs=(P(None, axis_name), P()),
        check_vma=False,
    )
```

```python
import functools

import jax
import jax.numpy as jnp
from jax import lax
from jax.sharding import PartitionSpec as P
from jax.experimental import pallas as pl
from jax.experimental.pallas import tpu as pltpu

N = 16
NV = 15680
NVP = 15744
D = 1024
B = 256
J = 128
RB = B // N
R = 1024
NMAIN = NV // R
TAIL = NV - NMAIN * R
TAILP = NVP - NMAIN * R
NF = 2
LOG2E = 1.4426950408889634
MESH = pl.DeviceIdType.MESH
NT = (((1,), (1,)), ((), ()))


def lane_gather(x, idx):
    dn = lax.GatherDimensionNumbers(
        offset_dims=(), collapsed_slice_dims=(1,), start_index_map=(1,),
        operand_batching_dims=(0,), start_indices_batching_dims=(0,))
    return lax.gather(x, idx[:, :, None], dn, slice_sizes=(1, 1),
                      mode=lax.GatherScatterMode.PROMISE_IN_BOUNDS)


def reduce_list(f, xs):
    while len(xs) > 1:
        xs = [f(xs[i], xs[i + 1]) if i + 1 < len(xs) else xs[i] for i in range(0, len(xs), 2)]
    return xs[0]


def take_chunk(z_ref, col, tile0, ntiles, masked, k2, m_ref, s_ref, loc_ref, acc_ref):
    for g in range(B // 8):
        rows = slice(g * 8, g * 8 + 8)
        us = [z_ref[rows, pl.ds(col + k * 128, 128)] for k in range(ntiles)]
        loc = loc_ref[rows, :]
        ti = (loc >> 7) - tile0
        li = loc & 127
        acc = acc_ref[rows, :]
        for k, u in enumerate(us):
            acc = jnp.where(ti == k, lane_gather(u, li), acc)
        acc_ref[rows, :] = acc
        if masked:
            lane = lax.broadcasted_iota(jnp.int32, (8, 128), 1)
            us[-1] = jnp.where(lane < NV % 128, us[-1], -jnp.inf)
        m = m_ref[rows, :]
        mn = jnp.maximum(m, reduce_list(jnp.maximum, us))
        ps = [jnp.exp2((u - mn) * k2) for u in us]
        s_ref[rows, :] = s_ref[rows, :] * jnp.exp2((m - mn) * k2) + reduce_list(jnp.add, ps)
        m_ref[rows, :] = mn


def head_kernel(t_ref, x_hbm, w_ref, b_ref, e_hbm, c_hbm, z_ref, lz_ref, q_ref,
                ebuf, xbuf, abuf, loc, m_ref, s_ref, cacc, st_send, st_recv, rs_recv, ag_send, ag_recv,
                esem, xsem, csem, st_ss, st_rs, rs_ss, rs_rs, ag_ss, ag_rs):
    me = lax.axis_index("vp")
    peers = [lax.rem(me + k, N) for k in range(1, N)]

    xcp = pltpu.make_async_copy(x_hbm, xbuf, xsem)
    xcp.start()
    ccp = pltpu.make_async_copy(c_hbm, loc, csem)
    ccp.start()

    def ecp(c):
        o = pl.multiple_of(c * R, R)
        return pltpu.make_async_copy(e_hbm.at[pl.ds(o, R)], ebuf.at[pl.ds(o, R)], esem.at[c])

    tcp = pltpu.make_async_copy(e_hbm.at[pl.ds(NMAIN * R, TAIL)], ebuf.at[pl.ds(NMAIN * R, TAIL)], esem.at[NMAIN])
    for c in range(NF):
        ecp(c).start()

    bar = pltpu.get_barrier_semaphore()
    for p in peers:
        pl.semaphore_signal(bar, inc=1, device_id=(p,), device_id_type=MESH)

    ebuf[NV:NVP, :] = jnp.zeros((NVP - NV, D), jnp.bfloat16)
    m_ref[...] = jnp.full_like(m_ref, -jnp.inf)
    s_ref[...] = jnp.zeros_like(s_ref)
    cacc[...] = jnp.zeros_like(cacc)
    inv_t = 1.0 / t_ref[...]
    k2 = inv_t * LOG2E

    xcp.wait()
    for c in range(NF, NMAIN):
        ecp(c).start()
    tcp.start()

    wv = w_ref[...].astype(jnp.float32).reshape(1, D)
    bv = b_ref[...].astype(jnp.float32).reshape(1, D)
    for g in range(0, B, 64):
        x = xbuf[g:g + 64, :].astype(jnp.float32)
        mu = jnp.sum(x, axis=1, keepdims=True) * (1.0 / D)
        xc = x - mu
        var = jnp.sum(xc * xc, axis=1, keepdims=True) * (1.0 / D)
        abuf[g:g + 64, :] = (xc * lax.rsqrt(var + 1e-5) * wv + bv).astype(jnp.bfloat16)

    ccp.wait()
    lv = loc[...] - me * NV
    loc[...] = jnp.where((lv >= 0) & (lv < NV), lv, -1)

    def mm(c):
        o = pl.multiple_of(c * R, R)
        return lax.dot_general(abuf[...], ebuf[pl.ds(o, R), :], NT, preferred_element_type=jnp.float32)

    ecp(0).wait()
    z_ref[:, 0:R] = mm(0)

    def step(c, carry):
        ecp(c).wait()
        z = mm(c)
        o = pl.multiple_of(c * R, R)
        take_chunk(z_ref, o - R, (c - 1) * (R // 128), R // 128, False, k2, m_ref, s_ref, loc, cacc)
        z_ref[:, pl.ds(o, R)] = z
        return carry

    lax.fori_loop(1, NMAIN, step, 0)
    tcp.wait()
    z = lax.dot_general(abuf[...], ebuf[NMAIN * R:NVP, :], NT, preferred_element_type=jnp.float32)
    take_chunk(z_ref, (NMAIN - 1) * R, (NMAIN - 1) * (R // 128), R // 128, False, k2, m_ref, s_ref, loc, cacc)
    z_ref[:, NMAIN * R:NVP] = z
    take_chunk(z_ref, NMAIN * R, NMAIN * (R // 128), TAILP // 128, True, k2, m_ref, s_ref, loc, cacc)

    mt = m_ref[...].T
    mloc = jnp.max(mt, axis=0, keepdims=True)
    sloc = jnp.sum(s_ref[...].T * jnp.exp2((mt - mloc) * k2), axis=0, keepdims=True)
    st_send[0:1, :] = mloc
    st_send[1:2, :] = sloc
    pl.semaphore_wait(bar, N - 1)

    st = []
    for k in range(1, N):
        cp = pltpu.make_async_remote_copy(st_send, st_recv.at[k], st_ss.at[k], st_rs.at[k], device_id=(peers[k - 1],), device_id_type=MESH)
        cp.start()
        st.append(cp)
    rs = []
    for k in range(1, N):
        cp = pltpu.make_async_remote_copy(cacc.at[pl.ds(pl.multiple_of(peers[k - 1] * RB, RB), RB)], rs_recv.at[k], rs_ss.at[k], rs_rs.at[k],
                                          device_id=(peers[k - 1],), device_id_type=MESH)
        cp.start()
        rs.append(cp)
    for cp in st:
        cp.wait()
    mp = [mloc] + [st_recv[k, 0:1, :] for k in range(1, N)]
    sp = [sloc] + [st_recv[k, 1:2, :] for k in range(1, N)]
    mg = functools.reduce(jnp.maximum, mp)
    sg = functools.reduce(jnp.add, [b * jnp.exp2((a - mg) * k2) for a, b in zip(mp, sp)])
    lz = mg * inv_t + jnp.log(sg)
    lz_ref[...] = lz
    for cp in rs:
        cp.wait()
    tot = cacc[pl.ds(pl.multiple_of(me * RB, RB), RB), :]
    for k in range(1, N):
        tot = tot + rs_recv[k]
    ag_send[...] = tot
    ag = []
    for k in range(1, N):
        cp = pltpu.make_async_remote_copy(ag_send, ag_recv.at[pl.ds(pl.multiple_of(me * RB, RB), RB)], ag_ss.at[k], ag_rs.at[k],
                                          device_id=(peers[k - 1],), device_id_type=MESH)
        cp.start()
        ag.append(cp)
    cols = [jnp.broadcast_to(lz[:, ih * 128:(ih + 1) * 128], (128, 128)).T for ih in range(2)]
    for cp in ag:
        cp.wait()
    ag_recv[pl.ds(pl.multiple_of(me * RB, RB), RB), :] = tot
    for ih in range(2):
        q_ref[ih * 128:(ih + 1) * 128, :] = ag_recv[ih * 128:(ih + 1) * 128, :] * inv_t - cols[ih]


WB = 640
WSLOT = 4


def write_kernel(t_ref, z_ref, lz_ref, q_ref, lp_hbm, q_hbm, buf, sems, qsem):
    qcp = pltpu.make_async_copy(q_ref, q_hbm, qsem)
    qcp.start()
    inv_t = 1.0 / t_ref[...]
    lz = lz_ref[...]
    cps = []
    n = NV // WB
    sizes = [WB] * n + ([NV - n * WB] if NV % WB else [])
    o = 0
    for c, r in enumerate(sizes):
        s = c % WSLOT
        if c >= WSLOT:
            cps[c - WSLOT].wait()
        rp = -(-r // 128) * 128
        zt = z_ref[:, o:o + rp].T
        buf[s, 0:r, :] = zt[0:r, :] * inv_t - lz
        cp = pltpu.make_async_copy(buf.at[s, pl.ds(0, r)], lp_hbm.at[pl.ds(o, r)], sems.at[c])
        cp.start()
        cps.append(cp)
        o += r
    for cp in cps[-WSLOT:]:
        cp.wait()
    qcp.wait()


def solution(mesh):
    axis_name = mesh.axis_names[0]
    vm = pl.BlockSpec(memory_space=pltpu.VMEM)
    anyspec = pl.BlockSpec(memory_space=pl.ANY)

    def per_device(hidden, ln_weight, ln_bias, emb_shard, temperature, cand_ids):
        t11 = temperature.reshape(1, 1)
        z, lz, q = pl.pallas_call(
            head_kernel,
            out_shape=[pltpu.VMEM((B, NVP), jnp.float32), pltpu.VMEM((1, B), jnp.float32), pltpu.VMEM((B, J), jnp.float32)],
            in_specs=[vm, anyspec, vm, vm, anyspec, anyspec],
            out_specs=[vm] * 3,
            scratch_shapes=[
                pltpu.VMEM((NVP, D), jnp.bfloat16),
                pltpu.VMEM((B, D), jnp.bfloat16),
                pltpu.VMEM((B, D), jnp.bfloat16),
                pltpu.VMEM((B, J), jnp.int32),
                pltpu.VMEM((B, 128), jnp.float32),
                pltpu.VMEM((B, 128), jnp.float32),
                pltpu.VMEM((B, J), jnp.float32),
                pltpu.VMEM((2, B), jnp.float32),
                pltpu.VMEM((N, 2, B), jnp.float32),
                pltpu.VMEM((N, RB, J), jnp.float32),
                pltpu.VMEM((RB, J), jnp.float32),
                pltpu.VMEM((B, J), jnp.float32),
                pltpu.SemaphoreType.DMA((NMAIN + 1,)),
                pltpu.SemaphoreType.DMA,
                pltpu.SemaphoreType.DMA,
                pltpu.SemaphoreType.DMA((N,)),
                pltpu.SemaphoreType.DMA((N,)),
                pltpu.SemaphoreType.DMA((N,)),
                pltpu.SemaphoreType.DMA((N,)),
                pltpu.SemaphoreType.DMA((N,)),
                pltpu.SemaphoreType.DMA((N,)),
            ],
            compiler_params=pltpu.CompilerParams(collective_id=0, has_side_effects=True, vmem_limit_bytes=44 * 1024 * 1024),
        )(t11, hidden, ln_weight, ln_bias, emb_shard, cand_ids)
        pin = lambda a: pltpu.with_memory_space_constraint(a, pltpu.VMEM)
        nw = -(-NV // WB)
        lp, qo = pl.pallas_call(
            write_kernel,
            out_shape=[jax.ShapeDtypeStruct((NV, B), jnp.float32), jax.ShapeDtypeStruct((B, J), jnp.float32)],
            in_specs=[vm] * 4,
            out_specs=[anyspec] * 2,
            scratch_shapes=[
                pltpu.VMEM((WSLOT, WB, B), jnp.float32),
                pltpu.SemaphoreType.DMA((nw,)),
                pltpu.SemaphoreType.DMA,
            ],
            compiler_params=pltpu.CompilerParams(vmem_limit_bytes=24 * 1024 * 1024),
        )(t11, pin(z), pin(lz), pin(q))
        return lp.T, qo

    return jax.shard_map(
        per_device,
        mesh=mesh,
        in_specs=(P(), P(), P(), P(axis_name, None), P(), P()),
        out_specs=(P(None, axis_name), P()),
        check_vma=False,
    )
```

```python
import functools

import jax
import jax.numpy as jnp
from jax import lax
from jax.sharding import PartitionSpec as P
from jax.experimental import pallas as pl
from jax.experimental.pallas import tpu as pltpu

N = 16
NV = 15680
NVP = 15744
D = 1024
B = 256
J = 128
RB = B // N
R = 1024
NMAIN = NV // R
TAIL = NV - NMAIN * R
TAILP = NVP - NMAIN * R
NF = 2
LOG2E = 1.4426950408889634
MESH = pl.DeviceIdType.MESH
NT = (((1,), (1,)), ((), ()))


def lane_gather(x, idx):
    dn = lax.GatherDimensionNumbers(
        offset_dims=(), collapsed_slice_dims=(1,), start_index_map=(1,),
        operand_batching_dims=(0,), start_indices_batching_dims=(0,))
    return lax.gather(x, idx[:, :, None], dn, slice_sizes=(1, 1),
                      mode=lax.GatherScatterMode.PROMISE_IN_BOUNDS)


def reduce_list(f, xs):
    while len(xs) > 1:
        xs = [f(xs[i], xs[i + 1]) if i + 1 < len(xs) else xs[i] for i in range(0, len(xs), 2)]
    return xs[0]


def take_chunk(z_ref, tile0, ntiles, masked, k2, m_ref, s_ref, loc_ref, acc_ref):
    for g in range(B // 8):
        rows = slice(g * 8, g * 8 + 8)
        us = [z_ref[rows, k * 128:(k + 1) * 128] for k in range(ntiles)]
        loc = loc_ref[rows, :]
        ti = (loc >> 7) - tile0
        li = loc & 127
        acc = acc_ref[rows, :]
        for k, u in enumerate(us):
            acc = jnp.where(ti == k, lane_gather(u, li), acc)
        acc_ref[rows, :] = acc
        if masked:
            lane = lax.broadcasted_iota(jnp.int32, (8, 128), 1)
            us[-1] = jnp.where(lane < NV % 128, us[-1], -jnp.inf)
        m = m_ref[rows, :]
        mn = jnp.maximum(m, reduce_list(jnp.maximum, us))
        ps = [jnp.exp2((u - mn) * k2) for u in us]
        s_ref[rows, :] = s_ref[rows, :] * jnp.exp2((m - mn) * k2) + reduce_list(jnp.add, ps)
        m_ref[rows, :] = mn


def head_kernel(t_ref, x_hbm, w_ref, b_ref, e_hbm, c_hbm, z_ref, lz_ref, q_ref,
                ebuf, xbuf, abuf, zs, loc, m_ref, s_ref, cacc, st_send, st_recv, rs_recv, ag_send, ag_recv,
                esem, xsem, csem, st_ss, st_rs, rs_ss, rs_rs, ag_ss, ag_rs):
    me = lax.axis_index("vp")
    peers = [lax.rem(me + k, N) for k in range(1, N)]

    xcp = pltpu.make_async_copy(x_hbm, xbuf, xsem)
    xcp.start()
    ccp = pltpu.make_async_copy(c_hbm, loc, csem)
    ccp.start()

    def ecp(c):
        o = pl.multiple_of(c * R, R)
        return pltpu.make_async_copy(e_hbm.at[pl.ds(o, R)], ebuf.at[pl.ds(o, R)], esem.at[c])

    tcp = pltpu.make_async_copy(e_hbm.at[pl.ds(NMAIN * R, TAIL)], ebuf.at[pl.ds(NMAIN * R, TAIL)], esem.at[NMAIN])
    for c in range(NF):
        ecp(c).start()

    bar = pltpu.get_barrier_semaphore()
    for p in peers:
        pl.semaphore_signal(bar, inc=1, device_id=(p,), device_id_type=MESH)

    ebuf[NV:NVP, :] = jnp.zeros((NVP - NV, D), jnp.bfloat16)
    m_ref[...] = jnp.full_like(m_ref, -jnp.inf)
    s_ref[...] = jnp.zeros_like(s_ref)
    cacc[...] = jnp.zeros_like(cacc)
    inv_t = 1.0 / t_ref[...]
    k2 = inv_t * LOG2E

    xcp.wait()
    for c in range(NF, NMAIN):
        ecp(c).start()
    tcp.start()

    wv = w_ref[...].astype(jnp.float32).reshape(1, D)
    bv = b_ref[...].astype(jnp.float32).reshape(1, D)
    for g in range(0, B, 64):
        x = xbuf[g:g + 64, :].astype(jnp.float32)
        mu = jnp.sum(x, axis=1, keepdims=True) * (1.0 / D)
        xc = x - mu
        var = jnp.sum(xc * xc, axis=1, keepdims=True) * (1.0 / D)
        abuf[g:g + 64, :] = (xc * lax.rsqrt(var + 1e-5) * wv + bv).astype(jnp.bfloat16)

    ccp.wait()
    lv = loc[...] - me * NV
    loc[...] = jnp.where((lv >= 0) & (lv < NV), lv, -1)

    def mm(c):
        o = pl.multiple_of(c * R, R)
        return lax.dot_general(abuf[...], ebuf[pl.ds(o, R), :], NT, preferred_element_type=jnp.float32)

    def take(slot, c):
        take_chunk(zs.at[slot], c * (R // 128), R // 128, False, k2, m_ref, s_ref, loc, cacc)

    def put(slot, c, z):
        zs[slot] = z
        z_ref[:, pl.ds(pl.multiple_of(c * R, R), R)] = z

    ecp(0).wait()
    put(0, 0, mm(0))

    def step(i, carry):
        for d in range(2):
            c = 1 + 2 * i + d
            ecp(c).wait()
            z = mm(c)
            take(d, c - 1)
            put(1 - d, c, z)
        return carry

    lax.fori_loop(0, (NMAIN - 1) // 2, step, 0)
    tcp.wait()
    z = lax.dot_general(abuf[...], ebuf[NMAIN * R:NVP, :], NT, preferred_element_type=jnp.float32)
    take(0, NMAIN - 1)
    zs[1, :, 0:TAILP] = z
    z_ref[:, NMAIN * R:NVP] = z
    take_chunk(zs.at[1], NMAIN * (R // 128), TAILP // 128, True, k2, m_ref, s_ref, loc, cacc)

    mt = m_ref[...].T
    mloc = jnp.max(mt, axis=0, keepdims=True)
    sloc = jnp.sum(s_ref[...].T * jnp.exp2((mt - mloc) * k2), axis=0, keepdims=True)
    st_send[0:1, :] = mloc
    st_send[1:2, :] = sloc
    pl.semaphore_wait(bar, N - 1)

    st = []
    for k in range(1, N):
        cp = pltpu.make_async_remote_copy(st_send, st_recv.at[k], st_ss.at[k], st_rs.at[k], device_id=(peers[k - 1],), device_id_type=MESH)
        cp.start()
        st.append(cp)
    rs = []
    for k in range(1, N):
        cp = pltpu.make_async_remote_copy(cacc.at[pl.ds(pl.multiple_of(peers[k - 1] * RB, RB), RB)], rs_recv.at[k], rs_ss.at[k], rs_rs.at[k],
                                          device_id=(peers[k - 1],), device_id_type=MESH)
        cp.start()
        rs.append(cp)
    for cp in st:
        cp.wait()
    mp = [mloc] + [st_recv[k, 0:1, :] for k in range(1, N)]
    sp = [sloc] + [st_recv[k, 1:2, :] for k in range(1, N)]
    mg = functools.reduce(jnp.maximum, mp)
    sg = functools.reduce(jnp.add, [b * jnp.exp2((a - mg) * k2) for a, b in zip(mp, sp)])
    lz = mg * inv_t + jnp.log(sg)
    lz_ref[...] = lz
    for cp in rs:
        cp.wait()
    tot = cacc[pl.ds(pl.multiple_of(me * RB, RB), RB), :]
    for k in range(1, N):
        tot = tot + rs_recv[k]
    ag_send[...] = tot
    ag = []
    for k in range(1, N):
        cp = pltpu.make_async_remote_copy(ag_send, ag_recv.at[pl.ds(pl.multiple_of(me * RB, RB), RB)], ag_ss.at[k], ag_rs.at[k],
                                          device_id=(peers[k - 1],), device_id_type=MESH)
        cp.start()
        ag.append(cp)
    cols = [jnp.broadcast_to(lz[:, ih * 128:(ih + 1) * 128], (128, 128)).T for ih in range(2)]
    for cp in ag:
        cp.wait()
    ag_recv[pl.ds(pl.multiple_of(me * RB, RB), RB), :] = tot
    for ih in range(2):
        q_ref[ih * 128:(ih + 1) * 128, :] = ag_recv[ih * 128:(ih + 1) * 128, :] * inv_t - cols[ih]


WB = 640


def write_kernel(t_ref, z_ref, lz_ref, q_ref, lp_hbm, q_hbm, buf, sems, qsem):
    qcp = pltpu.make_async_copy(q_ref, q_hbm, qsem)
    qcp.start()
    inv_t = 1.0 / t_ref[...]
    lz = lz_ref[...]
    cps = []
    for c, o in enumerate(range(0, NV, WB)):
        r = min(WB, NV - o)
        rp = -(-r // 128) * 128
        zt = z_ref[:, o:o + rp].T
        buf[o:o + r, :] = zt[0:r, :] * inv_t - lz
        cp = pltpu.make_async_copy(buf.at[pl.ds(o, r)], lp_hbm.at[pl.ds(o, r)], sems.at[c])
        cp.start()
        cps.append(cp)
    for cp in cps:
        cp.wait()
    qcp.wait()


def solution(mesh):
    axis_name = mesh.axis_names[0]
    vm = pl.BlockSpec(memory_space=pltpu.VMEM)
    anyspec = pl.BlockSpec(memory_space=pl.ANY)

    def per_device(hidden, ln_weight, ln_bias, emb_shard, temperature, cand_ids):
        t11 = temperature.reshape(1, 1)
        z, lz, q = pl.pallas_call(
            head_kernel,
            out_shape=[pltpu.VMEM((B, NVP), jnp.float32), pltpu.VMEM((1, B), jnp.float32), pltpu.VMEM((B, J), jnp.float32)],
            in_specs=[vm, anyspec, vm, vm, anyspec, anyspec],
            out_specs=[vm] * 3,
            scratch_shapes=[
                pltpu.VMEM((NVP, D), jnp.bfloat16),
                pltpu.VMEM((B, D), jnp.bfloat16),
                pltpu.VMEM((B, D), jnp.bfloat16),
                pltpu.VMEM((2, B, R), jnp.float32),
                pltpu.VMEM((B, J), jnp.int32),
                pltpu.VMEM((B, 128), jnp.float32),
                pltpu.VMEM((B, 128), jnp.float32),
                pltpu.VMEM((B, J), jnp.float32),
                pltpu.VMEM((2, B), jnp.float32),
                pltpu.VMEM((N, 2, B), jnp.float32),
                pltpu.VMEM((N, RB, J), jnp.float32),
                pltpu.VMEM((RB, J), jnp.float32),
                pltpu.VMEM((B, J), jnp.float32),
                pltpu.SemaphoreType.DMA((NMAIN + 1,)),
                pltpu.SemaphoreType.DMA,
                pltpu.SemaphoreType.DMA,
                pltpu.SemaphoreType.DMA((N,)),
                pltpu.SemaphoreType.DMA((N,)),
                pltpu.SemaphoreType.DMA((N,)),
                pltpu.SemaphoreType.DMA((N,)),
                pltpu.SemaphoreType.DMA((N,)),
                pltpu.SemaphoreType.DMA((N,)),
            ],
            compiler_params=pltpu.CompilerParams(collective_id=0, has_side_effects=True, vmem_limit_bytes=44 * 1024 * 1024),
        )(t11, hidden, ln_weight, ln_bias, emb_shard, cand_ids)
        pin = lambda a: pltpu.with_memory_space_constraint(a, pltpu.VMEM)
        nw = -(-NV // WB)
        lp, qo = pl.pallas_call(
            write_kernel,
            out_shape=[jax.ShapeDtypeStruct((NV, B), jnp.float32), jax.ShapeDtypeStruct((B, J), jnp.float32)],
            in_specs=[vm] * 4,
            out_specs=[anyspec] * 2,
            scratch_shapes=[
                pltpu.VMEM((NV, B), jnp.float32),
                pltpu.SemaphoreType.DMA((nw,)),
                pltpu.SemaphoreType.DMA,
            ],
            compiler_params=pltpu.CompilerParams(vmem_limit_bytes=24 * 1024 * 1024),
        )(t11, pin(z), pin(lz), pin(q))
        return lp.T, qo

    return jax.shard_map(
        per_device,
        mesh=mesh,
        in_specs=(P(), P(), P(), P(axis_name, None), P(), P()),
        out_specs=(P(None, axis_name), P()),
        check_vma=False,
    )
```

```python
import functools

import jax
import jax.numpy as jnp
from jax import lax
from jax.sharding import PartitionSpec as P
from jax.experimental import pallas as pl
from jax.experimental.pallas import tpu as pltpu

N = 16
NV = 15680
NVP = 15744
D = 1024
B = 256
J = 128
RB = B // N
R = 1024
NMAIN = NV // R
TAIL = NV - NMAIN * R
TAILP = NVP - NMAIN * R
KS = 512
NF = 2
LOG2E = 1.4426950408889634
MESH = pl.DeviceIdType.MESH
NT = (((1,), (1,)), ((), ()))


def lane_gather(x, idx):
    dn = lax.GatherDimensionNumbers(
        offset_dims=(), collapsed_slice_dims=(1,), start_index_map=(1,),
        operand_batching_dims=(0,), start_indices_batching_dims=(0,))
    return lax.gather(x, idx[:, :, None], dn, slice_sizes=(1, 1),
                      mode=lax.GatherScatterMode.PROMISE_IN_BOUNDS)


def reduce_list(f, xs):
    while len(xs) > 1:
        xs = [f(xs[i], xs[i + 1]) if i + 1 < len(xs) else xs[i] for i in range(0, len(xs), 2)]
    return xs[0]


def take_chunk(z_ref, tile0, ntiles, masked, k2, m_ref, s_ref, loc_ref, acc_ref):
    for g in range(B // 8):
        rows = slice(g * 8, g * 8 + 8)
        us = [z_ref[rows, k * 128:(k + 1) * 128] for k in range(ntiles)]
        loc = loc_ref[rows, :]
        ti = (loc >> 7) - tile0
        li = loc & 127
        acc = acc_ref[rows, :]
        for k, u in enumerate(us):
            acc = jnp.where(ti == k, lane_gather(u, li), acc)
        acc_ref[rows, :] = acc
        if masked:
            lane = lax.broadcasted_iota(jnp.int32, (8, 128), 1)
            us[-1] = jnp.where(lane < NV % 128, us[-1], -jnp.inf)
        m = m_ref[rows, :]
        mn = jnp.maximum(m, reduce_list(jnp.maximum, us))
        ps = [jnp.exp2((u - mn) * k2) for u in us]
        s_ref[rows, :] = s_ref[rows, :] * jnp.exp2((m - mn) * k2) + reduce_list(jnp.add, ps)
        m_ref[rows, :] = mn


def head_kernel(t_ref, x_hbm, w_hbm, b_hbm, e_hbm, c_hbm, z_ref, lz_ref, q_ref,
                ebuf, xbuf, w_ref, b_ref, abuf, zs, loc, m_ref, s_ref, cacc, st_send, st_recv, rs_recv, ag_send, ag_recv,
                esem, xsem, wsem, bsem, csem, st_ss, st_rs, rs_ss, rs_rs, ag_ss, ag_rs):
    me = lax.axis_index("vp")
    peers = [lax.rem(me + k, N) for k in range(1, N)]

    xcp = pltpu.make_async_copy(x_hbm, xbuf, xsem)
    xcp.start()
    wcp = pltpu.make_async_copy(w_hbm, w_ref, wsem)
    wcp.start()
    bcp = pltpu.make_async_copy(b_hbm, b_ref, bsem)
    bcp.start()
    ccp = pltpu.make_async_copy(c_hbm, loc, csem)
    ccp.start()

    def ecp(c):
        o = pl.multiple_of(c * R, R)
        return pltpu.make_async_copy(e_hbm.at[pl.ds(o, R)], ebuf.at[pl.ds(o, R)], esem.at[c])

    tcp = pltpu.make_async_copy(e_hbm.at[pl.ds(NMAIN * R, TAIL)], ebuf.at[pl.ds(NMAIN * R, TAIL)], esem.at[NMAIN])
    for c in range(NF):
        ecp(c).start()

    bar = pltpu.get_barrier_semaphore()
    for p in peers:
        pl.semaphore_signal(bar, inc=1, device_id=(p,), device_id_type=MESH)

    ebuf[NV:NVP, :] = jnp.zeros((NVP - NV, D), jnp.bfloat16)
    m_ref[...] = jnp.full_like(m_ref, -jnp.inf)
    s_ref[...] = jnp.zeros_like(s_ref)
    cacc[...] = jnp.zeros_like(cacc)
    inv_t = 1.0 / t_ref[...]
    k2 = inv_t * LOG2E

    xcp.wait()
    wcp.wait()
    bcp.wait()
    for c in range(NF, NMAIN):
        ecp(c).start()
    tcp.start()

    wv = w_ref[...].astype(jnp.float32).reshape(1, D)
    bv = b_ref[...].astype(jnp.float32).reshape(1, D)
    for g in range(0, B, 64):
        x = xbuf[g:g + 64, :].astype(jnp.float32)
        mu = jnp.sum(x, axis=1, keepdims=True) * (1.0 / D)
        xc = x - mu
        var = jnp.sum(xc * xc, axis=1, keepdims=True) * (1.0 / D)
        abuf[g:g + 64, :] = (xc * lax.rsqrt(var + 1e-5) * wv + bv).astype(jnp.bfloat16)

    ccp.wait()
    lv = loc[...] - me * NV
    loc[...] = jnp.where((lv >= 0) & (lv < NV), lv, -1)

    def dots(o, r):
        parts = [lax.dot_general(abuf[:, j:j + KS], ebuf[pl.ds(o, r), j:j + KS], NT, preferred_element_type=jnp.float32)
                 for j in range(0, D, KS)]
        return functools.reduce(jnp.add, parts)

    def mm(c):
        o = pl.multiple_of(c * R, R)
        return dots(o, R)

    def take(slot, c):
        take_chunk(zs.at[slot], c * (R // 128), R // 128, False, k2, m_ref, s_ref, loc, cacc)

    def put(slot, c, z):
        zs[slot] = z
        z_ref[:, pl.ds(pl.multiple_of(c * R, R), R)] = z

    ecp(0).wait()
    put(0, 0, mm(0))

    def step(i, carry):
        for d in range(2):
            c = 1 + 2 * i + d
            ecp(c).wait()
            z = mm(c)
            take(d, c - 1)
            put(1 - d, c, z)
        return carry

    lax.fori_loop(0, (NMAIN - 1) // 2, step, 0)
    tcp.wait()
    z = dots(NMAIN * R, TAILP)
    take(0, NMAIN - 1)
    zs[1, :, 0:TAILP] = z
    z_ref[:, NMAIN * R:NVP] = z
    take_chunk(zs.at[1], NMAIN * (R // 128), TAILP // 128, True, k2, m_ref, s_ref, loc, cacc)

    mt = m_ref[...].T
    mloc = jnp.max(mt, axis=0, keepdims=True)
    sloc = jnp.sum(s_ref[...].T * jnp.exp2((mt - mloc) * k2), axis=0, keepdims=True)
    st_send[0:1, :] = mloc
    st_send[1:2, :] = sloc
    pl.semaphore_wait(bar, N - 1)

    st = []
    for k in range(1, N):
        cp = pltpu.make_async_remote_copy(st_send, st_recv.at[k], st_ss.at[k], st_rs.at[k], device_id=(peers[k - 1],), device_id_type=MESH)
        cp.start()
        st.append(cp)
    rs = []
    for k in range(1, N):
        cp = pltpu.make_async_remote_copy(cacc.at[pl.ds(pl.multiple_of(peers[k - 1] * RB, RB), RB)], rs_recv.at[k], rs_ss.at[k], rs_rs.at[k],
                                          device_id=(peers[k - 1],), device_id_type=MESH)
        cp.start()
        rs.append(cp)
    for cp in st:
        cp.wait()
    mp = [mloc] + [st_recv[k, 0:1, :] for k in range(1, N)]
    sp = [sloc] + [st_recv[k, 1:2, :] for k in range(1, N)]
    mg = functools.reduce(jnp.maximum, mp)
    sg = functools.reduce(jnp.add, [b * jnp.exp2((a - mg) * k2) for a, b in zip(mp, sp)])
    lz = mg * inv_t + jnp.log(sg)
    lz_ref[...] = lz
    for cp in rs:
        cp.wait()
    tot = cacc[pl.ds(pl.multiple_of(me * RB, RB), RB), :]
    for k in range(1, N):
        tot = tot + rs_recv[k]
    ag_send[...] = tot
    ag = []
    for k in range(1, N):
        cp = pltpu.make_async_remote_copy(ag_send, ag_recv.at[pl.ds(pl.multiple_of(me * RB, RB), RB)], ag_ss.at[k], ag_rs.at[k],
                                          device_id=(peers[k - 1],), device_id_type=MESH)
        cp.start()
        ag.append(cp)
    cols = [jnp.broadcast_to(lz[:, ih * 128:(ih + 1) * 128], (128, 128)).T for ih in range(2)]
    for cp in ag:
        cp.wait()
    ag_recv[pl.ds(pl.multiple_of(me * RB, RB), RB), :] = tot
    for ih in range(2):
        q_ref[ih * 128:(ih + 1) * 128, :] = ag_recv[ih * 128:(ih + 1) * 128, :] * inv_t - cols[ih]


WB = 640


def write_kernel(t_ref, z_ref, lz_ref, q_ref, lp_hbm, q_hbm, buf, sems, qsem):
    qcp = pltpu.make_async_copy(q_ref, q_hbm, qsem)
    qcp.start()
    inv_t = 1.0 / t_ref[...]
    lz = lz_ref[...]
    cps = []
    for c, o in enumerate(range(0, NV, WB)):
        r = min(WB, NV - o)
        rp = -(-r // 128) * 128
        zt = z_ref[:, o:o + rp].T
        buf[o:o + r, :] = zt[0:r, :] * inv_t - lz
        cp = pltpu.make_async_copy(buf.at[pl.ds(o, r)], lp_hbm.at[pl.ds(o, r)], sems.at[c])
        cp.start()
        cps.append(cp)
    for cp in cps:
        cp.wait()
    qcp.wait()


def solution(mesh):
    axis_name = mesh.axis_names[0]
    vm = pl.BlockSpec(memory_space=pltpu.VMEM)
    anyspec = pl.BlockSpec(memory_space=pl.ANY)

    def per_device(hidden, ln_weight, ln_bias, emb_shard, temperature, cand_ids):
        t11 = temperature.reshape(1, 1)
        z, lz, q = pl.pallas_call(
            head_kernel,
            out_shape=[pltpu.VMEM((B, NVP), jnp.float32), pltpu.VMEM((1, B), jnp.float32), pltpu.VMEM((B, J), jnp.float32)],
            in_specs=[vm, anyspec, anyspec, anyspec, anyspec, anyspec],
            out_specs=[vm] * 3,
            scratch_shapes=[
                pltpu.VMEM((NVP, D), jnp.bfloat16),
                pltpu.VMEM((B, D), jnp.bfloat16),
                pltpu.VMEM((D,), jnp.bfloat16),
                pltpu.VMEM((D,), jnp.bfloat16),
                pltpu.VMEM((B, D), jnp.bfloat16),
                pltpu.VMEM((2, B, R), jnp.float32),
                pltpu.VMEM((B, J), jnp.int32),
                pltpu.VMEM((B, 128), jnp.float32),
                pltpu.VMEM((B, 128), jnp.float32),
                pltpu.VMEM((B, J), jnp.float32),
                pltpu.VMEM((2, B), jnp.float32),
                pltpu.VMEM((N, 2, B), jnp.float32),
                pltpu.VMEM((N, RB, J), jnp.float32),
                pltpu.VMEM((RB, J), jnp.float32),
                pltpu.VMEM((B, J), jnp.float32),
                pltpu.SemaphoreType.DMA((NMAIN + 1,)),
                pltpu.SemaphoreType.DMA,
                pltpu.SemaphoreType.DMA,
                pltpu.SemaphoreType.DMA,
                pltpu.SemaphoreType.DMA,
                pltpu.SemaphoreType.DMA((N,)),
                pltpu.SemaphoreType.DMA((N,)),
                pltpu.SemaphoreType.DMA((N,)),
                pltpu.SemaphoreType.DMA((N,)),
                pltpu.SemaphoreType.DMA((N,)),
                pltpu.SemaphoreType.DMA((N,)),
            ],
            compiler_params=pltpu.CompilerParams(collective_id=0, has_side_effects=True, vmem_limit_bytes=44 * 1024 * 1024),
        )(t11, hidden, ln_weight, ln_bias, emb_shard, cand_ids)
        pin = lambda a: pltpu.with_memory_space_constraint(a, pltpu.VMEM)
        nw = -(-NV // WB)
        lp, qo = pl.pallas_call(
            write_kernel,
            out_shape=[jax.ShapeDtypeStruct((NV, B), jnp.float32), jax.ShapeDtypeStruct((B, J), jnp.float32)],
            in_specs=[vm] * 4,
            out_specs=[anyspec] * 2,
            scratch_shapes=[
                pltpu.VMEM((NV, B), jnp.float32),
                pltpu.SemaphoreType.DMA((nw,)),
                pltpu.SemaphoreType.DMA,
            ],
            compiler_params=pltpu.CompilerParams(vmem_limit_bytes=24 * 1024 * 1024),
        )(t11, pin(z), pin(lz), pin(q))
        return lp.T, qo

    return jax.shard_map(
        per_device,
        mesh=mesh,
        in_specs=(P(), P(), P(), P(axis_name, None), P(), P()),
        out_specs=(P(None, axis_name), P()),
        check_vma=False,
    )
```

```python
import functools

import jax
import jax.numpy as jnp
from jax import lax
from jax.sharding import PartitionSpec as P
from jax.experimental import pallas as pl
from jax.experimental.pallas import tpu as pltpu

N = 16
NV = 15680
NVP = 15744
D = 1024
B = 256
J = 128
RB = B // N
R = 1024
NMAIN = NV // R
TAIL = NV - NMAIN * R
TAILP = NVP - NMAIN * R
KS = 512
NF = 2
LOG2E = 1.4426950408889634
MESH = pl.DeviceIdType.MESH
NT = (((1,), (1,)), ((), ()))


def lane_gather(x, idx):
    dn = lax.GatherDimensionNumbers(
        offset_dims=(), collapsed_slice_dims=(1,), start_index_map=(1,),
        operand_batching_dims=(0,), start_indices_batching_dims=(0,))
    return lax.gather(x, idx[:, :, None], dn, slice_sizes=(1, 1),
                      mode=lax.GatherScatterMode.PROMISE_IN_BOUNDS)


def reduce_list(f, xs):
    while len(xs) > 1:
        xs = [f(xs[i], xs[i + 1]) if i + 1 < len(xs) else xs[i] for i in range(0, len(xs), 2)]
    return xs[0]


def take_candidates(us, rows, tile0, loc_ref, acc_ref):
    loc = loc_ref[rows, :]
    ti = (loc >> 7) - tile0
    li = loc & 127
    acc = acc_ref[rows, :]
    for k, u in enumerate(us):
        acc = jnp.where(ti == k, lane_gather(u, li), acc)
    acc_ref[rows, :] = acc


def take_stats(us, rows, masked, k2, m_ref, s_ref):
    if masked:
        lane = lax.broadcasted_iota(jnp.int32, (8, 128), 1)
        us = us[:-1] + [jnp.where(lane < NV % 128, us[-1], -jnp.inf)]
    m = m_ref[rows, :]
    mn = jnp.maximum(m, reduce_list(jnp.maximum, us))
    ps = [jnp.exp2((u - mn) * k2) for u in us]
    s_ref[rows, :] = s_ref[rows, :] * jnp.exp2((m - mn) * k2) + reduce_list(jnp.add, ps)
    m_ref[rows, :] = mn


def row_groups(z_ref, ntiles):
    for g in range(B // 8):
        rows = slice(g * 8, g * 8 + 8)
        yield rows, [z_ref[rows, k * 128:(k + 1) * 128] for k in range(ntiles)]


def head_kernel(t_hbm, x_hbm, w_hbm, b_hbm, e_hbm, c_hbm, z_ref, lz_ref, q_ref,
                ebuf, xbuf, t_ref, w_ref, b_ref, abuf, zs, loc, m_ref, s_ref, cacc, st_send, st_recv, rs_recv, ag_send, ag_recv,
                esem, xsem, tsem, wsem, bsem, csem, st_ss, st_rs, rs_ss, rs_rs, ag_ss, ag_rs):
    me = lax.axis_index("vp")
    peers = [lax.rem(me + k, N) for k in range(1, N)]

    xcp = pltpu.make_async_copy(x_hbm, xbuf, xsem)
    xcp.start()
    tmcp = pltpu.make_async_copy(t_hbm, t_ref, tsem)
    tmcp.start()
    wcp = pltpu.make_async_copy(w_hbm, w_ref, wsem)
    wcp.start()
    bcp = pltpu.make_async_copy(b_hbm, b_ref, bsem)
    bcp.start()
    ccp = pltpu.make_async_copy(c_hbm, loc, csem)
    ccp.start()

    def ecp(c):
        o = pl.multiple_of(c * R, R)
        return pltpu.make_async_copy(e_hbm.at[pl.ds(o, R)], ebuf.at[pl.ds(o, R)], esem.at[c])

    tcp = pltpu.make_async_copy(e_hbm.at[pl.ds(NMAIN * R, TAIL)], ebuf.at[pl.ds(NMAIN * R, TAIL)], esem.at[NMAIN])
    for c in range(NF):
        ecp(c).start()

    bar = pltpu.get_barrier_semaphore()
    for p in peers:
        pl.semaphore_signal(bar, inc=1, device_id=(p,), device_id_type=MESH)

    ebuf[NV:NVP, :] = jnp.zeros((NVP - NV, D), jnp.bfloat16)
    m_ref[...] = jnp.full_like(m_ref, -jnp.inf)
    s_ref[...] = jnp.zeros_like(s_ref)
    cacc[...] = jnp.zeros_like(cacc)
    xcp.wait()
    wcp.wait()
    bcp.wait()
    for c in range(NF, NMAIN):
        ecp(c).start()
    tcp.start()

    wv = w_ref[...].astype(jnp.float32).reshape(1, D)
    bv = b_ref[...].astype(jnp.float32).reshape(1, D)
    for g in range(0, B, 64):
        x = xbuf[g:g + 64, :].astype(jnp.float32)
        mu = jnp.sum(x, axis=1, keepdims=True) * (1.0 / D)
        xc = x - mu
        var = jnp.sum(xc * xc, axis=1, keepdims=True) * (1.0 / D)
        abuf[g:g + 64, :] = (xc * lax.rsqrt(var + 1e-5) * wv + bv).astype(jnp.bfloat16)

    ccp.wait()
    tmcp.wait()
    inv_t = 1.0 / t_ref[...]
    k2 = inv_t * LOG2E
    lv = loc[...] - me * NV
    loc[...] = jnp.where((lv >= 0) & (lv < NV), lv, -1)

    def dots(o, r):
        parts = [lax.dot_general(abuf[:, j:j + KS], ebuf[pl.ds(o, r), j:j + KS], NT, preferred_element_type=jnp.float32)
                 for j in range(0, D, KS)]
        return functools.reduce(jnp.add, parts)

    def mm(c):
        o = pl.multiple_of(c * R, R)
        return dots(o, R)

    def take(slot, c):
        for rows, us in row_groups(zs.at[slot], R // 128):
            take_candidates(us, rows, c * (R // 128), loc, cacc)
            take_stats(us, rows, False, k2, m_ref, s_ref)

    def put(slot, c, z):
        zs[slot] = z
        z_ref[:, pl.ds(pl.multiple_of(c * R, R), R)] = z

    ecp(0).wait()
    put(0, 0, mm(0))

    def step(i, carry):
        for d in range(2):
            c = 1 + 2 * i + d
            ecp(c).wait()
            z = mm(c)
            take(d, c - 1)
            put(1 - d, c, z)
        return carry

    lax.fori_loop(0, (NMAIN - 1) // 2, step, 0)
    tcp.wait()
    z = dots(NMAIN * R, TAILP)
    for rows, us in row_groups(zs.at[0], R // 128):
        take_candidates(us, rows, (NMAIN - 1) * (R // 128), loc, cacc)
    zs[1, :, 0:TAILP] = z
    z_ref[:, NMAIN * R:NVP] = z
    for rows, us in row_groups(zs.at[1], TAILP // 128):
        take_candidates(us, rows, NMAIN * (R // 128), loc, cacc)
    pl.semaphore_wait(bar, N - 1)

    rs = []
    for k in range(1, N):
        cp = pltpu.make_async_remote_copy(cacc.at[pl.ds(pl.multiple_of(peers[k - 1] * RB, RB), RB)], rs_recv.at[k], rs_ss.at[k], rs_rs.at[k],
                                          device_id=(peers[k - 1],), device_id_type=MESH)
        cp.start()
        rs.append(cp)

    for rows, us in row_groups(zs.at[0], R // 128):
        take_stats(us, rows, False, k2, m_ref, s_ref)
    for rows, us in row_groups(zs.at[1], TAILP // 128):
        take_stats(us, rows, True, k2, m_ref, s_ref)
    mt = m_ref[...].T
    mloc = jnp.max(mt, axis=0, keepdims=True)
    sloc = jnp.sum(s_ref[...].T * jnp.exp2((mt - mloc) * k2), axis=0, keepdims=True)
    st_send[0:1, :] = mloc
    st_send[1:2, :] = sloc
    st = []
    for k in range(1, N):
        cp = pltpu.make_async_remote_copy(st_send, st_recv.at[k], st_ss.at[k], st_rs.at[k], device_id=(peers[k - 1],), device_id_type=MESH)
        cp.start()
        st.append(cp)

    for cp in rs:
        cp.wait()
    tot = cacc[pl.ds(pl.multiple_of(me * RB, RB), RB), :]
    for k in range(1, N):
        tot = tot + rs_recv[k]
    ag_send[...] = tot
    ag = []
    for k in range(1, N):
        cp = pltpu.make_async_remote_copy(ag_send, ag_recv.at[pl.ds(pl.multiple_of(me * RB, RB), RB)], ag_ss.at[k], ag_rs.at[k],
                                          device_id=(peers[k - 1],), device_id_type=MESH)
        cp.start()
        ag.append(cp)
    for cp in st:
        cp.wait()
    mp = [mloc] + [st_recv[k, 0:1, :] for k in range(1, N)]
    sp = [sloc] + [st_recv[k, 1:2, :] for k in range(1, N)]
    mg = functools.reduce(jnp.maximum, mp)
    sg = functools.reduce(jnp.add, [b * jnp.exp2((a - mg) * k2) for a, b in zip(mp, sp)])
    lz = mg * inv_t + jnp.log(sg)
    lz_ref[0:1, :] = lz
    lz_ref[1:2, :] = jnp.broadcast_to(inv_t, (1, B))
    cols = [jnp.broadcast_to(lz[:, ih * 128:(ih + 1) * 128], (128, 128)).T for ih in range(2)]
    for cp in ag:
        cp.wait()
    ag_recv[pl.ds(pl.multiple_of(me * RB, RB), RB), :] = tot
    for ih in range(2):
        q_ref[ih * 128:(ih + 1) * 128, :] = ag_recv[ih * 128:(ih + 1) * 128, :] * inv_t - cols[ih]


WB = 640


def write_kernel(z_ref, lz_ref, q_ref, lp_hbm, q_hbm, buf, sems, qsem):
    qcp = pltpu.make_async_copy(q_ref, q_hbm, qsem)
    qcp.start()
    lz = lz_ref[0:1, :]
    inv_t = lz_ref[1:2, :]
    cps = []
    for c, o in enumerate(range(0, NV, WB)):
        r = min(WB, NV - o)
        rp = -(-r // 128) * 128
        zt = z_ref[:, o:o + rp].T
        buf[o:o + r, :] = zt[0:r, :] * inv_t - lz
        cp = pltpu.make_async_copy(buf.at[pl.ds(o, r)], lp_hbm.at[pl.ds(o, r)], sems.at[c])
        cp.start()
        cps.append(cp)
    for cp in cps:
        cp.wait()
    qcp.wait()


def solution(mesh):
    axis_name = mesh.axis_names[0]
    vm = pl.BlockSpec(memory_space=pltpu.VMEM)
    anyspec = pl.BlockSpec(memory_space=pl.ANY)

    def per_device(hidden, ln_weight, ln_bias, emb_shard, temperature, cand_ids):
        t11 = temperature.reshape(1, 1)
        z, lz, q = pl.pallas_call(
            head_kernel,
            out_shape=[pltpu.VMEM((B, NVP), jnp.float32), pltpu.VMEM((2, B), jnp.float32), pltpu.VMEM((B, J), jnp.float32)],
            in_specs=[anyspec, anyspec, anyspec, anyspec, anyspec, anyspec],
            out_specs=[vm] * 3,
            scratch_shapes=[
                pltpu.VMEM((NVP, D), jnp.bfloat16),
                pltpu.VMEM((B, D), jnp.bfloat16),
                pltpu.VMEM((1, 1), jnp.float32),
                pltpu.VMEM((D,), jnp.bfloat16),
                pltpu.VMEM((D,), jnp.bfloat16),
                pltpu.VMEM((B, D), jnp.bfloat16),
                pltpu.VMEM((2, B, R), jnp.float32),
                pltpu.VMEM((B, J), jnp.int32),
                pltpu.VMEM((B, 128), jnp.float32),
                pltpu.VMEM((B, 128), jnp.float32),
                pltpu.VMEM((B, J), jnp.float32),
                pltpu.VMEM((2, B), jnp.float32),
                pltpu.VMEM((N, 2, B), jnp.float32),
                pltpu.VMEM((N, RB, J), jnp.float32),
                pltpu.VMEM((RB, J), jnp.float32),
                pltpu.VMEM((B, J), jnp.float32),
                pltpu.SemaphoreType.DMA((NMAIN + 1,)),
                pltpu.SemaphoreType.DMA,
                pltpu.SemaphoreType.DMA,
                pltpu.SemaphoreType.DMA,
                pltpu.SemaphoreType.DMA,
                pltpu.SemaphoreType.DMA,
                pltpu.SemaphoreType.DMA((N,)),
                pltpu.SemaphoreType.DMA((N,)),
                pltpu.SemaphoreType.DMA((N,)),
                pltpu.SemaphoreType.DMA((N,)),
                pltpu.SemaphoreType.DMA((N,)),
                pltpu.SemaphoreType.DMA((N,)),
            ],
            compiler_params=pltpu.CompilerParams(collective_id=0, has_side_effects=True, vmem_limit_bytes=44 * 1024 * 1024),
        )(t11, hidden, ln_weight, ln_bias, emb_shard, cand_ids)
        pin = lambda a: pltpu.with_memory_space_constraint(a, pltpu.VMEM)
        nw = -(-NV // WB)
        lp, qo = pl.pallas_call(
            write_kernel,
            out_shape=[jax.ShapeDtypeStruct((NV, B), jnp.float32), jax.ShapeDtypeStruct((B, J), jnp.float32)],
            in_specs=[vm] * 3,
            out_specs=[anyspec] * 2,
            scratch_shapes=[
                pltpu.VMEM((NV, B), jnp.float32),
                pltpu.SemaphoreType.DMA((nw,)),
                pltpu.SemaphoreType.DMA,
            ],
            compiler_params=pltpu.CompilerParams(vmem_limit_bytes=24 * 1024 * 1024),
        )(pin(z), pin(lz), pin(q))
        return lp.T, qo

    return jax.shard_map(
        per_device,
        mesh=mesh,
        in_specs=(P(), P(), P(), P(axis_name, None), P(), P()),
        out_specs=(P(None, axis_name), P()),
        check_vma=False,
    )
```
